256 devices in a mesh: ctx: 8 (over z), vocab: 32 (over y, x, core).
Axes of the slice: x: 4, y: 4, z: 8, core: 2. Of those that a mesh axis runs over, the one named last changes fastest.
Arguments:
- hidden: bfloat16 [16, 128, 4096], P(None, 'ctx', 'vocab'), may hold values from -6 to 6
- head_weight: bfloat16 [4096, 128256], P(None, ('ctx', 'vocab')), may hold values from -0.09375 to 0.09375
- token_ids: int32 [16, 128], P(None, 'ctx'), may hold values from 0 to 128255
- response_mask: int32 [16, 128], P(None, 'ctx'), may hold values 0 or 1
- pair_order: int32 [16], replicated, may hold values from 0 to 15, each once
- frozen_logprob: float32 [16], replicated, may hold values from -40 to 40
Outputs:
- pair_loss: float32 [], replicated
- margins: float32 [8], replicated
- head_grad: bfloat16 [4096, 128256], P(None, ('ctx', 'vocab'))
- spread_grad: bfloat16 [4096, 128256], P(None, ('ctx', 'vocab'))
The draws below stay inside these ranges and needn't reach their ends.
Inputs may be any that keep to these rules, and one draw needn't show every extreme that they name: `token_ids`: token ids lie in 0 to 128255. `response_mask`: mask entries are 0 or 1. pair_order names every sequence exactly once; entry p is the chosen sequence of pair p and entry 8 + p the rejected one.
All inputs are finite; a program needn't handle non-finite values.
Results may differ from the reference program's by a relative error of at most 0.0015.
Values may be sent and summed in bfloat16 or wider, within the bound.
A program may use at most 128 MiB of HBM per device.

```python
import jax
import jax.numpy as jnp

D = 4096
V = 128256
PAIRS = 8
SEQS = 16
LENGTH = 128


def touch_ends(entries, own_key, least, top_value):
    shape = entries.shape
    index_at = [jax.random.randint(jax.random.fold_in(own_key, axis), (), 0, shape[axis]) for axis in range(len(shape))]
    entries = entries.at[tuple(index_at)].set(least)
    longest = shape.index(max(shape))
    index_at[longest] = (index_at[longest] + 1) % shape[longest]
    return entries.at[tuple(index_at)].set(top_value)


def steps_of(key, shape, shards, low, largest):
    def one(position, parts):
        steps = jax.random.uniform(jax.random.fold_in(jax.random.fold_in(key, 6), position), (parts,), jnp.float32, low / len(shards), largest / len(shards))
        return jnp.repeat(jnp.exp(steps), shape[position] // parts).reshape((-1,) + (1,) * (len(shape) - position - 1))

    level = one(*shards[0])
    for cut in shards[1:]:
        level = level * one(*cut)
    return level


def gaussian(stream_key, dims, spread, reach, pieces=(), dtype=jnp.bfloat16):
    values = jax.random.normal(stream_key, dims, jnp.float32) * spread
    if len(pieces) > 0:
        values = steps_of(stream_key, dims, pieces, -0.22, 0.18) * values
    return jnp.clip(values, min=-reach, max=reach).astype(dtype)


def setup_inputs(seed: int = 0) -> dict:
    splits = jax.random.split(jax.random.key(seed), 7)
    hidden = gaussian(splits[0], (SEQS, LENGTH, D), 1.0, 6.0, ((1, 8), (2, 32)))
    head_weight = gaussian(splits[1], (D, V), D ** -0.5, 0.09375, ((1, 256),))
    token_ids = touch_ends(jax.random.randint(splits[2], (SEQS, LENGTH), 0, V), jax.random.fold_in(splits[2], 1), 0, V - 1).astype(jnp.int32)
    response_mask = touch_ends((jax.random.randint(splits[3], (SEQS, LENGTH), 0, 8) < 7).astype(jnp.int32), jax.random.fold_in(splits[3], 1), 0, 1)
    pair_order = jax.random.permutation(splits[4], SEQS).astype(jnp.int32)
    frozen_logprob = gaussian(splits[5], (SEQS,), 8.0, 40.0, (), jnp.float32)
    return dict(hidden=hidden, head_weight=head_weight, token_ids=token_ids, response_mask=response_mask, pair_order=pair_order, frozen_logprob=frozen_logprob)


strength = 0.1
loss_scale = 256.0


def reference(hidden, head_weight, token_ids, response_mask, pair_order, frozen_logprob):
    token_rows = hidden.reshape(SEQS * LENGTH, D)
    logits = jnp.dot(token_rows, head_weight, preferred_element_type=jnp.float32)
    row_peak = jnp.max(logits, axis=1)
    log_norm = row_peak + jnp.log(jnp.sum(jnp.exp(logits - row_peak[:, None]), axis=1))
    flat_ids = token_ids.reshape(-1).astype(jnp.int32)
    picked = jnp.take_along_axis(logits, flat_ids[:, None], axis=1)[:, 0]
    mask_flat = response_mask.reshape(-1).astype(jnp.float32)
    policy = jnp.sum(((picked - log_norm) * mask_flat).reshape(SEQS, LENGTH), axis=1)
    log_ratio = policy - frozen_logprob
    chosen = pair_order[:PAIRS]
    rejected = pair_order[PAIRS:]
    margins = strength * (log_ratio[chosen] - log_ratio[rejected])
    pair_loss = jnp.mean(jax.nn.softplus(-margins))
    weight = -loss_scale * strength * jax.nn.sigmoid(-margins) / PAIRS
    seq_coef = jnp.zeros((SEQS,), jnp.float32).at[chosen].set(weight).at[rejected].set(-weight)
    token_coef = (seq_coef[:, None] * response_mask.astype(jnp.float32)).reshape(-1)
    probabilities = jnp.exp(logits - log_norm[:, None])
    columns = jnp.arange(V).astype(jnp.int32)
    onehot = (columns[None, :] == flat_ids[:, None]).astype(jnp.float32)
    grad_logits = (token_coef[:, None] * (onehot - probabilities)).astype(jnp.bfloat16)
    spread_logits = ((V / 64.0) * token_coef[:, None] * probabilities).astype(jnp.bfloat16)
    head_grad = jnp.dot(token_rows.T, grad_logits, preferred_element_type=jnp.float32).astype(jnp.bfloat16)
    spread_grad = jnp.dot(token_rows.T, spread_logits, preferred_element_type=jnp.float32).astype(jnp.bfloat16)
    return pair_loss, margins, head_grad, spread_grad
```

```python
import functools

import jax
import jax.numpy as jnp
from jax import lax
from jax.experimental import pallas as pl
from jax.experimental.pallas import tpu as pltpu
from jax.sharding import Mesh
from jax.sharding import PartitionSpec as P

V = 128256
NX, NY, NZ, NC = 4, 4, 8, 2
AX, AY, AZ, AC = "vocab_1", "vocab_0", "ctx", "vocab_2"
VOCAB = (AY, AX, AC)
CTX_VOCAB = (AZ,) + VOCAB
MESH = pl.DeviceIdType.MESH

SEQS = 16
PER = 4
CHUNKS = SEQS // PER
PAIRS = SEQS // 2
ROWS = 16
LENGTH = ROWS * NZ
LANES = 128
CHIPS = NX * NY
WIDTH = 501
PAD = 512

strength = 0.1
loss_scale = 256.0


def kind_of(s):
    q, j = divmod(s, PER)
    if j == 2:
        return "z"
    if j == 3:
        return "x" if q % 2 == 0 else "y"
    return "xy"[j]


def kernel(
    hid_ref, w_hbm, ids_ref, mask_ref, order_ref, frozen_ref,
    loss_ref, margins_ref, head_hbm, spread_hbm,
    held, w_ref, acc, logits, both, staged, meta, stats, cols, masks, turn,
    w_sem, r1, r2, r3, s1, s2, s3, pair_r, pair_s, meta_r, meta_s, stat_r, stat_s, out_sem,
):
    x = lax.axis_index(AX)
    y = lax.axis_index(AY)
    z = lax.axis_index(AZ)
    c = lax.axis_index(AC)
    place = y * NX + x
    shard = ((z * NY + y) * NX + x) * NC + c

    w_copy = pltpu.make_async_copy(w_hbm, w_ref, w_sem)
    w_copy.start()

    def peer(axis, step):
        index, size = {AX: (x, NX), AY: (y, NY), AZ: (z, NZ), AC: (c, NC)}[axis]
        return {axis: lax.rem(index + step + size, size)}

    def send(ref, send_sem, recv_sem, to):
        pltpu.make_async_remote_copy(
            src_ref=ref, dst_ref=ref, send_sem=send_sem, recv_sem=recv_sem,
            device_id=to, device_id_type=MESH,
        ).start()

    def arrived(ref, sem):
        pltpu.make_async_copy(ref, ref, sem).wait()

    def across(ref, s):
        send(ref, pair_s.at[s // PER], pair_r.at[s // PER], peer(AC, 1))

    for j in range(SEQS):
        seq = order_ref[j // 2 + (j % 2) * PAIRS]
        held[j, place, c, pl.ds(z * ROWS, ROWS), :] = hid_ref[seq]
    turn[...] = jnp.zeros_like(turn)
    for j in range(SEQS):
        seq = order_ref[j // 2 + (j % 2) * PAIRS]
        turn[pl.ds(j, 1), 0:ROWS] = ids_ref[pl.ds(seq, 1), :].astype(jnp.float32)
        turn[pl.ds(SEQS + j, 1), 0:ROWS] = mask_ref[pl.ds(seq, 1), :].astype(jnp.float32)
    meta[pl.ds(z * ROWS, ROWS), :] = turn[...].T[0:ROWS, :]

    barrier = pltpu.get_barrier_semaphore()
    greeted = 0
    for axis, size in ((AX, NX), (AY, NY), (AZ, NZ), (AC, NC)):
        for step in range(1, size):
            pl.semaphore_signal(barrier, inc=1, device_id=peer(axis, step), device_id_type=MESH)
            greeted += 1
    pl.semaphore_wait(barrier, greeted)

    def axes_of(s):
        return (AY, AX) if kind_of(s) == "x" else (AX, AY)

    def line(s, i2, i3):
        if kind_of(s) == "x":
            row, col = lax.rem(y + i2, NY), lax.rem(x + i3, NX)
        else:
            row, col = lax.rem(y + i3, NY), lax.rem(x + i2, NX)
        return held.at[s, row * NX + col, c]

    def half(ref, side):
        return ref.at[pl.ds(side * (LENGTH // 2), LENGTH // 2), :]

    def own_rows(step=0):
        return pl.ds(lax.rem(z + step + NZ, NZ) * ROWS, ROWS)

    def bar(s, i2, side=None):
        row = lax.rem(y + i2, NY) * NX
        if side is None:
            return held.at[s, pl.ds(row, NX), c, own_rows(), :]
        return held.at[s, pl.ds(row + side * 2, 2), c, own_rows(), :]

    def plane(s, i3, side=None):
        if side is None:
            return held.at[s, :, c, own_rows(i3), :]
        return held.at[s, pl.ds(side * (CHIPS // 2), CHIPS // 2), c, own_rows(i3), :]

    def third(s, k):
        a3 = axes_of(s)[1]
        ref = line(s, k, 0)
        send(ref, s3.at[s], r3.at[s, 4 * k], peer(a3, 1))
        send(ref, s3.at[s], r3.at[s, 4 * k + 1], peer(a3, -1))
        across(ref, s)

    def round_a(s):
        ref = held.at[s, place, c, own_rows(), :]
        axis, size = (AX, NX) if kind_of(s) == "z" else (AZ, NZ)
        for step in range(1, size):
            send(ref, s1.at[s], r1.at[s], peer(axis, step))

    def round_b(s):
        if kind_of(s) == "z":
            arrived(held.at[s, 0, 0, pl.ds(0, (NX - 1) * ROWS), :], r1.at[s])
            ref = bar(s, 0)
            send(ref, s2.at[s], r2.at[s, 0], peer(AY, 1))
            send(ref, s2.at[s], r2.at[s, 1], peer(AY, -1))
        else:
            arrived(held.at[s, 0, 0, pl.ds(0, (NZ - 1) * ROWS), :], r1.at[s])
            a2 = axes_of(s)[0]
            ref = line(s, 0, 0)
            send(ref, s2.at[s], r2.at[s, 0], peer(a2, 1))
            send(ref, s2.at[s], r2.at[s, 1], peer(a2, -1))
            third(s, 0)

    def round_c(s):
        if kind_of(s) == "z":
            arrived(bar(s, 3), r2.at[s, 0])
            send(bar(s, 3, 0), s2.at[s], r2.at[s, 2], peer(AY, 1))
            arrived(bar(s, 1), r2.at[s, 1])
            send(bar(s, 1, 1), s2.at[s], r2.at[s, 3], peer(AY, -1))
        else:
            a2 = axes_of(s)[0]
            arrived(line(s, 3, 0), r2.at[s, 0])
            send(half(line(s, 3, 0), 0), s2.at[s], r2.at[s, 2], peer(a2, 1))
            third(s, 3)
            arrived(line(s, 1, 0), r2.at[s, 1])
            send(half(line(s, 1, 0), 1), s2.at[s], r2.at[s, 3], peer(a2, -1))
            third(s, 1)

    def round_d(s):
        if kind_of(s) == "z":
            arrived(bar(s, 2, 0), r2.at[s, 2])
            arrived(bar(s, 2, 1), r2.at[s, 3])
            ref = plane(s, 0)
            send(ref, s3.at[s], r3.at[s, 0], peer(AZ, 1))
            send(ref, s3.at[s], r3.at[s, 4], peer(AZ, -1))
            across(ref, s)
        else:
            arrived(half(line(s, 2, 0), 0), r2.at[s, 2])
            arrived(half(line(s, 2, 0), 1), r2.at[s, 3])
            third(s, 2)

    def ring_of_four(s, k):
        a3 = axes_of(s)[1]
        arrived(line(s, k, 3), r3.at[s, 4 * k])
        send(half(line(s, k, 3), 0), s3.at[s], r3.at[s, 4 * k + 2], peer(a3, 1))
        across(line(s, k, 3), s)
        arrived(line(s, k, 1), r3.at[s, 4 * k + 1])
        send(half(line(s, k, 1), 1), s3.at[s], r3.at[s, 4 * k + 3], peer(a3, -1))
        across(line(s, k, 1), s)

    def ring_of_eight(s, d):
        left, right = plane(s, -d), plane(s, d)
        arrived(left, r3.at[s, d - 1])
        send(left if d < 3 else plane(s, -d, 0), s3.at[s], r3.at[s, d], peer(AZ, 1))
        across(left, s)
        arrived(right, r3.at[s, 3 + d])
        send(right if d < 3 else plane(s, d, 1), s3.at[s], r3.at[s, 4 + d], peer(AZ, -1))
        across(right, s)

    def round_e(s):
        if kind_of(s) == "z":
            ring_of_eight(s, 1)
        else:
            ring_of_four(s, 0)

    def round_f(s):
        if kind_of(s) == "z":
            ring_of_eight(s, 2)
        else:
            ring_of_four(s, 3)
            ring_of_four(s, 1)

    def round_g(s):
        if kind_of(s) == "z":
            ring_of_eight(s, 3)
        else:
            ring_of_four(s, 2)

    def round_h(s):
        if kind_of(s) == "z":
            arrived(plane(s, 4, 0), r3.at[s, 3])
            arrived(plane(s, 4, 1), r3.at[s, 7])
            across(plane(s, 4), s)
        else:
            for k in (0, 3, 1, 2):
                arrived(half(line(s, k, 2), 0), r3.at[s, 4 * k + 2])
                arrived(half(line(s, k, 2), 1), r3.at[s, 4 * k + 3])
                across(line(s, k, 2), s)

    def chunk(q, step):
        if q < CHUNKS:
            for j in (2, 0, 1, 3):
                step(q * PER + j)

    def forward(q):
        @pl.loop(0, PER // 2)
        def _(i):
            s = q * PER + i * 2
            total = jnp.zeros((2 * LENGTH, WIDTH), jnp.float32)
            for k in range(CHIPS):
                lhs = jnp.concatenate(
                    [held[pl.ds(s, 2), k, e].reshape(2 * LENGTH, LANES) for e in range(NC)], axis=1
                )
                total += jnp.dot(
                    lhs, w_ref[pl.ds(k * NC * LANES, NC * LANES), :], preferred_element_type=jnp.float32
                )
            logits[pl.ds(s, 2)] = total.reshape(2, LENGTH, WIDTH)

    lane = lax.broadcasted_iota(jnp.int32, (LENGTH, LANES), 1)
    column = (lax.broadcasted_iota(jnp.int32, (LENGTH, WIDTH), 1) + shard * WIDTH).astype(jnp.float32)

    def local_stats(q):
        table = jnp.zeros((LENGTH, LANES), jnp.float32)
        for j in range(PER):
            s = q * PER + j
            part = logits[s]
            top = jnp.max(part, axis=1, keepdims=True)
            total = jnp.sum(jnp.exp(part - top), axis=1, keepdims=True)
            hit = column == meta[:, s : s + 1]
            target = jnp.sum(jnp.where(hit, part, 0.0), axis=1, keepdims=True)
            table = jnp.where(lane == j, top, table)
            table = jnp.where(lane == 8 + j, total, table)
            table = jnp.where(lane == 16 + j, target, table)
        return table.T[0:24, :]

    stages = ((AC, c, NC, 0), (AX, x, NX, 2), (AY, y, NY, 6), (AZ, z, NZ, 10))

    def share(q, stage, value):
        axis, index, size, at = stages[stage]
        ref = stats.at[q, at + index]
        ref[...] = value
        for step in range(1, size):
            send(ref, stat_s.at[q, stage], stat_r.at[q, stage], peer(axis, step))

    def merged(q, stage):
        axis, index, size, at = stages[stage]
        arrived(stats.at[q, pl.ds(0, size - 1)], stat_r.at[q, stage])
        parts = [stats[q, at + i] for i in range(size)]
        top = functools.reduce(jnp.maximum, [p[0:8] for p in parts])
        total = sum(p[8:16] * jnp.exp(p[0:8] - top) for p in parts)
        target = sum(p[16:24] for p in parts)
        return top, total, target

    def relay(q, stage):
        share(q, stage + 1, jnp.concatenate(merged(q, stage), axis=0))

    row8 = lax.broadcasted_iota(jnp.int32, (8, LANES), 0)

    def coefs(q, loss):
        top, total, target = merged(q, 3)
        log_norm = top + jnp.log(total)
        mask = masks[q]
        frozen = jnp.zeros((8, LANES), jnp.float32)
        for j in range(PER):
            seq = order_ref[q * 2 + j // 2 + (j % 2) * PAIRS]
            frozen = jnp.where(row8 == j, frozen_ref[seq], frozen)
        terms = jnp.where(row8 < PER, (target - log_norm) * mask, 0.0)
        ratio = jnp.sum(terms, axis=1, keepdims=True) - frozen
        even = row8 % 2 == 0
        after = jnp.concatenate([ratio[1:8], ratio[0:1]], axis=0)
        before = jnp.concatenate([ratio[7:8], ratio[0:7]], axis=0)
        margin = strength * jnp.where(even, ratio - after, before - ratio)
        tail = jnp.exp(-jnp.abs(margin))
        soft = jnp.maximum(-margin, 0.0) + jnp.log1p(tail)
        sigmoid = jnp.where(margin > 0, tail, 1.0) / (1.0 + tail)
        weight = -loss_scale * strength * sigmoid / PAIRS
        coef = jnp.where(even, weight, -weight) * mask
        for i in range(PER // 2):
            margins_ref[q * 2 + i] = jnp.max(margin[2 * i : 2 * i + 1, 0:1])
            loss = loss + jnp.max(soft[2 * i : 2 * i + 1, 0:1])
        table = jnp.concatenate(
            [log_norm, coef, jnp.zeros((LANES - 16, LANES), jnp.float32)], axis=0
        )
        cols[...] = table.T
        for j in range(PER):
            s = q * PER + j
            prob = jnp.exp(logits[s] - cols[:, j : j + 1])
            weight_col = cols[:, 8 + j : 9 + j]
            onehot = jnp.where(column == meta[:, s : s + 1], 1.0, 0.0)
            rows = pl.ds(j * LENGTH, LENGTH)
            both[rows, 0:WIDTH] = (weight_col * (onehot - prob)).astype(jnp.bfloat16)
            both[rows, PAD : PAD + WIDTH] = ((V / 64.0) * weight_col * prob).astype(jnp.bfloat16)
        return loss

    def backward(q, first, last):
        @pl.loop(first, last)
        def _(k):
            lhs = jnp.concatenate(
                [held[pl.ds(q * PER, PER), k, e].reshape(PER * LENGTH, LANES) for e in range(NC)], axis=1
            )
            part = lax.dot_general(
                lhs, both[...], (((0,), (0,)), ((), ())), preferred_element_type=jnp.float32
            )
            if q > 0:
                part = part + acc[k]
            if q < CHUNKS - 1:
                acc[k] = part
            else:
                rows = pl.ds(k * NC * LANES, NC * LANES)
                staged[0, k] = part[:, 0:WIDTH].astype(jnp.bfloat16)
                staged[1, k] = part[:, PAD : PAD + WIDTH].astype(jnp.bfloat16)
                pltpu.make_async_copy(staged.at[0, k], head_hbm.at[rows, :], out_sem.at[0]).start()
                pltpu.make_async_copy(staged.at[1, k], spread_hbm.at[rows, :], out_sem.at[1]).start()

    chunk(0, round_a)
    own_meta = meta.at[own_rows(), :]
    for step in range(1, NZ):
        send(own_meta, meta_s, meta_r, peer(AZ, step))
    chunk(1, round_a)
    both[...] = jnp.zeros_like(both)
    chunk(0, round_b)
    chunk(0, round_c)
    chunk(0, round_d)
    arrived(meta.at[pl.ds(0, (NZ - 1) * ROWS), :], meta_r)
    turned = meta[...].T
    for q in range(CHUNKS):
        rows = turned[SEQS + q * PER : SEQS + (q + 1) * PER]
        masks[q] = jnp.concatenate([rows, jnp.zeros((8 - PER, LANES), jnp.float32)], axis=0)
    w_copy.wait()
    loss = jnp.float32(0.0)
    for q in range(CHUNKS):
        chunk(q + 2, round_a)
        chunk(q + 1, round_b)
        chunk(q, round_e)
        if q > 0:
            relay(q - 1, 0)
        if q == 3:
            backward(0, 0, 6)
        chunk(q + 1, round_c)
        chunk(q, round_f)
        if q > 0:
            relay(q - 1, 1)
        if q == 3:
            backward(0, 6, 11)
        chunk(q + 1, round_d)
        chunk(q, round_g)
        if q > 0:
            relay(q - 1, 2)
        if q == 3:
            backward(0, 11, CHIPS)
        chunk(q, round_h)
        arrived(held.at[pl.ds(q * PER, PER), :, 0], pair_r.at[q])
        forward(q)
        share(q, 0, local_stats(q))
        if q == 1:
            loss = coefs(0, loss)
    loss = coefs(1, loss)
    relay(3, 0)
    backward(1, 0, 9)
    relay(3, 1)
    backward(1, 9, CHIPS)
    loss = coefs(2, loss)
    backward(2, 0, 2)
    relay(3, 2)
    backward(2, 2, CHIPS)
    loss = coefs(3, loss)
    backward(3, 0, CHIPS)
    loss_ref[0] = loss / PAIRS

    for s in range(SEQS):
        first = (NX if kind_of(s) == "z" else NZ) - 1
        arrived(held.at[s, 0, 0, pl.ds(0, first * ROWS), :], s1.at[s])
        if kind_of(s) == "z":
            arrived(held.at[s, pl.ds(0, 3), 0, pl.ds(0, LENGTH // 2), :], s2.at[s])
            arrived(held.at[s, pl.ds(0, 14), 0], s3.at[s])
        else:
            arrived(held.at[s, pl.ds(0, 3), 0], s2.at[s])
            arrived(held.at[s, pl.ds(0, 12), 0], s3.at[s])
    for q in range(CHUNKS):
        arrived(held.at[pl.ds(q * PER, PER), :, 0], pair_s.at[q])
        for stage in range(4):
            arrived(stats.at[q, pl.ds(0, stages[stage][2] - 1)], stat_s.at[q, stage])
    arrived(meta.at[pl.ds(0, (NZ - 1) * ROWS), :], meta_s)
    for i in range(2):
        arrived(staged.at[i], out_sem.at[i])


def shards(hidden, head_weight, token_ids, response_mask, pair_order, frozen_logprob):
    depth = head_weight.shape[0]
    vmem = pl.BlockSpec(memory_space=pltpu.VMEM)
    smem = pl.BlockSpec(memory_space=pltpu.SMEM)
    hbm = pl.BlockSpec(memory_space=pl.ANY)
    dma = pltpu.SemaphoreType.DMA
    loss, margins, head_grad, spread_grad = pl.pallas_call(
        kernel,
        out_shape=(
            jax.ShapeDtypeStruct((1,), jnp.float32),
            jax.ShapeDtypeStruct((PAIRS,), jnp.float32),
            jax.ShapeDtypeStruct((depth, WIDTH), jnp.bfloat16),
            jax.ShapeDtypeStruct((depth, WIDTH), jnp.bfloat16),
        ),
        in_specs=[vmem, hbm, vmem, vmem, smem, smem],
        out_specs=(smem, smem, hbm, hbm),
        scratch_shapes=[
            pltpu.VMEM((SEQS, CHIPS, NC, LENGTH, LANES), jnp.bfloat16),
            pltpu.VMEM((depth, WIDTH), jnp.bfloat16),
            pltpu.VMEM((CHIPS, NC * LANES, 2 * PAD), jnp.float32),
            pltpu.VMEM((SEQS, LENGTH, WIDTH), jnp.float32),
            pltpu.VMEM((PER * LENGTH, 2 * PAD), jnp.bfloat16),
            pltpu.VMEM((2, CHIPS, NC * LANES, WIDTH), jnp.bfloat16),
            pltpu.VMEM((LENGTH, LANES), jnp.float32),
            pltpu.VMEM((CHUNKS, 18, 24, LANES), jnp.float32),
            pltpu.VMEM((LENGTH, LANES), jnp.float32),
            pltpu.VMEM((CHUNKS, 8, LANES), jnp.float32),
            pltpu.VMEM((LANES, LANES), jnp.float32),
            dma,
            dma((SEQS,)),
            dma((SEQS, 4)),
            dma((SEQS, 16)),
            dma((SEQS,)),
            dma((SEQS,)),
            dma((SEQS,)),
            dma((CHUNKS,)),
            dma((CHUNKS,)),
            dma,
            dma,
            dma((CHUNKS, 4)),
            dma((CHUNKS, 4)),
            dma((2,)),
        ],
        compiler_params=pltpu.CompilerParams(
            collective_id=0, has_side_effects=True, vmem_limit_bytes=62 * 1024 * 1024
        ),
    )(hidden, head_weight, token_ids, response_mask, pair_order, frozen_logprob)
    return loss.reshape(()), margins, head_grad, spread_grad


def solution(mesh):
    split = Mesh(mesh.devices.reshape(NZ, NY, NX, NC), CTX_VOCAB)
    placed = (P(None, AZ, VOCAB), P(None, CTX_VOCAB), P(None, AZ), P(None, AZ), P(), P())
    return jax.shard_map(
        shards,
        mesh=split,
        in_specs=placed,
        out_specs=(P(), P(), P(None, CTX_VOCAB), P(None, CTX_VOCAB)),
        check_vma=False,
    )
```
